32 devices in a mesh: group: 8 (over z, x), peer: 4 (over y, core).
Axes of the slice: x: 2, y: 2, z: 4, core: 2. Of those that a mesh axis runs over, the one named last changes fastest.
Arguments:
- features: bfloat16 [12288, 1024], P(('group', 'peer')), may hold values from -6 to 6
- task_mask: int32 [12288], P(('group', 'peer')), may hold values from 0 to 65535, as said below
- tower_in: bfloat16 [16, 2048, 1024], P('peer', 'group'), may hold values from -0.1875 to 0.1875
- tower_bias: bfloat16 [16, 2048], P('peer', 'group'), may hold values from -5 to 5
- tower_head: bfloat16 [16, 2048], P('peer', 'group'), may hold values from -0.125 to 0.125
- head_bias: float32 [16], P('peer'), may hold values from -4 to 4
Outputs:
- predictions: float32 [12288, 16], P(('group', 'peer'))
The draws below stay inside these ranges and needn't reach their ends.
Inputs may be any that keep to these rules, and one draw needn't show every extreme that they name: `task_mask`: only bits 0 to 15 are used. Among the 384 samples of one device (aligned blocks of 384), at most 176 have any one bit set; in every run of 4 blocks that one group holds, some task's bit is set exactly 176 times in each block.
All inputs are finite; a program needn't handle non-finite values.
Results may differ from the reference program's by a relative error of at most 0.0003.
Values may be sent and summed in bfloat16 or wider, within the bound.
A program may use at most 128 MiB of HBM per device.

```python
import jax
import jax.numpy as jnp
from jax import lax

D = 1024
H = 2048
CAP = 176
SAMP_DEV = 384
TASKS = 16
SAMPLES = 12288
N_PEER = 4


def draw_task_mask(key, part):
    blocks = SAMPLES // SAMP_DEV
    groups = blocks // N_PEER
    hot_task = jax.random.randint(jax.random.fold_in(key, 11), (groups,), 0, TASKS)
    active_block = jnp.repeat(hot_task, N_PEER)
    spread = jax.random.randint(jax.random.fold_in(key, 12), (blocks, TASKS), 0, CAP + 1)
    counts = spread * spread // CAP
    task_ids = jnp.arange(TASKS, dtype=jnp.int32)
    counts = jnp.where(task_ids[None, :] == active_block[:, None], CAP, counts)
    keys = jax.random.split(jax.random.fold_in(key, 13), blocks * TASKS)
    sort_orders = jax.vmap(lambda single: jax.random.permutation(single, SAMP_DEV))(keys)
    sort_orders = sort_orders.reshape(blocks, TASKS, SAMP_DEV).astype(jnp.int32)
    task_bits = (sort_orders < counts[:, :, None]).astype(jnp.int32)
    packed = jnp.sum(task_bits << task_ids[None, :, None], axis=1)
    return packed.reshape(-1).astype(jnp.int32)


def levels(own_key, dims, cuts, low, top_value):
    def one(dim, blocks):
        steps = jax.random.uniform(jax.random.fold_in(jax.random.fold_in(own_key, 6), dim), (blocks,), jnp.float32, low / len(cuts), top_value / len(cuts))
        return jnp.repeat(jnp.exp(steps), dims[dim] // blocks).reshape((-1,) + (1,) * (len(dims) - dim - 1))

    level = one(*cuts[0])
    for cut in cuts[1:]:
        level = level * one(*cut)
    return level


def scatter_about(stream_key, extent, scale, limit, pieces=(), held_as=jnp.bfloat16):
    gain = levels(stream_key, extent, pieces, -0.22, 0.18) if pieces else 1.0
    values = jax.random.normal(stream_key, extent, jnp.float32) * scale * gain
    return jnp.minimum(jnp.maximum(values, -limit), limit).astype(held_as)


def setup_inputs(seed: int = 0) -> dict:
    key_list = jax.random.split(jax.random.key(seed), 7)
    features = scatter_about(key_list[0], (SAMPLES, D), 1.0, 6.0, ((0, 32),))
    task_mask = draw_task_mask(jax.random.fold_in(key_list[6], 71), 0)
    tower_in = scatter_about(key_list[2], (TASKS, H, D), D ** -0.5, 0.1875, ((0, 4), (1, 8)))
    tower_bias = scatter_about(key_list[3], (TASKS, H), 1.0, 5.0, ((0, 4), (1, 8)))
    tower_head = scatter_about(key_list[4], (TASKS, H), H ** -0.5, 0.125, ((0, 4), (1, 8)))
    head_bias = scatter_about(key_list[5], (TASKS,), 1.0, 4.0, ((0, 4),), jnp.float32)
    return dict(features=features, task_mask=task_mask, tower_in=tower_in, tower_bias=tower_bias, tower_head=tower_head, head_bias=head_bias)


def block_logits(block_rows, block_mask, layer_entry, hidden_unit_bias, head_rows, out_bias):
    sample_count = block_rows.shape[0]
    task_ids = jnp.arange(TASKS, dtype=jnp.int32)
    task_bits = (block_mask[:, None] >> task_ids[None, :]) & 1
    inclusive = jnp.cumsum(task_bits, axis=0)
    slot_rank = inclusive - task_bits
    slot_indices = jnp.arange(CAP, dtype=jnp.int32)
    sample_index = jnp.sum((inclusive[:, :, None] <= slot_indices[None, None, :]).astype(jnp.int32), axis=0)
    sample_index = jnp.clip(sample_index, 0, sample_count - 1).astype(jnp.int32)
    gathered = block_rows.astype(jnp.float32)[sample_index]
    preact = jnp.einsum("tcd,thd->tch", gathered, layer_entry, precision=lax.Precision.HIGHEST)
    hidden = jnp.maximum(preact + hidden_unit_bias[:, None, :], 0.0)
    logit = jnp.sum(hidden * head_rows[:, None, :], axis=-1) + out_bias[:, None]
    picked = logit[task_ids[None, :], jnp.clip(slot_rank, 0, CAP - 1).astype(jnp.int32)]
    return jnp.where(task_bits == 1, picked, jnp.float32(0.0))


def reference(features, task_mask, tower_in, tower_bias, tower_head, head_bias):
    blocks = SAMPLES // SAMP_DEV
    layer_entry = tower_in.astype(jnp.float32)
    hidden_unit_bias = tower_bias.astype(jnp.float32)
    head_rows = tower_head.astype(jnp.float32)
    rows_blocked = features.reshape(blocks, SAMP_DEV, D)
    mask_blocked = task_mask.reshape(blocks, SAMP_DEV)

    def one_block(pair):
        return block_logits(pair[0], pair[1], layer_entry, hidden_unit_bias, head_rows, head_bias)

    result = lax.map(one_block, (rows_blocked, mask_blocked))
    return result.reshape(SAMPLES, TASKS)
```

```python
import functools

import jax
import jax.numpy as jnp
from jax import lax
from jax.experimental import pallas as pl
from jax.experimental.pallas import tpu as pltpu
from jax.sharding import PartitionSpec as P

MESH = pl.DeviceIdType.MESH
LANES = 128
PIECES = 2
STEP_ROWS = 512
STEP_COLS = 256


def split_of_group(group, peers, weight_bytes, sample_bytes):
    sizes = [f for f in range(1, group + 1) if group % f == 0]

    def cost(f):
        return (f - 1) * weight_bytes + (group // f * peers - 1) * sample_bytes / 2

    return min(sizes, key=cost)


def kernel(
    outer, inner, peers,
    feat_ref, weight_ref, cols_ref, hbias_ref, out_ref,
    x_buf, w_buf, c_buf, part, ret,
    load_sem, x_recv, z_send, y_send, core_send, w_send, w_recv, c_send, c_recv, p_send, p_recv,
):
    rows, depth = feat_ref.shape
    towers, hidden, _ = weight_ref.shape
    piece = rows // PIECES
    ys = peers // 2
    group_at, me = lax.axis_index("group"), lax.axis_index("peer")
    a, i = group_at // inner, group_at % inner
    y, c = me // 2, me % 2
    partner = y * 2 + (1 - c)

    def dev(a_to, i_to, p_to):
        return (a_to * inner + i_to, p_to)

    load_x = pltpu.make_async_copy(
        feat_ref, x_buf.at[a, pl.ds(pl.multiple_of(me * rows, rows), rows)], load_sem.at[0]
    )
    load_w = pltpu.make_async_copy(weight_ref, w_buf.at[i], load_sem.at[1])
    load_c = pltpu.make_async_copy(cols_ref, c_buf.at[i], load_sem.at[2])
    load_x.start()
    load_w.start()
    load_c.start()

    barrier = pltpu.get_barrier_semaphore()
    others = outer * peers - 1

    def greet(k, _):
        at = lax.rem(a * peers + me + k, outer * peers)
        pl.semaphore_signal(
            barrier, inc=1, device_id=dev(at // peers, i, at % peers), device_id_type=MESH
        )
        return 0

    lax.fori_loop(1, others + 1, greet, 0)
    for k in range(1, inner):
        pl.semaphore_signal(
            barrier, inc=1, device_id=dev(a, lax.rem(i + k, inner), me), device_id_type=MESH
        )

    start = jnp.where(a == 0, hbias_ref[...], 0.0)
    for aa in range(outer):
        for pp in range(peers):
            part[aa, pp] = start

    load_x.wait()
    load_w.wait()
    load_c.wait()
    pl.semaphore_wait(barrier, others + inner - 1)

    def x_piece(aa, pp, h):
        return x_buf.at[aa, pl.ds(pl.multiple_of(pp * rows + h * piece, piece), piece)]

    def send_x(aa, pp, h, sem, to):
        ref = x_piece(aa, pp, h)
        return pltpu.make_async_remote_copy(
            src_ref=ref, dst_ref=ref, send_sem=sem, recv_sem=x_recv.at[aa, pp, h],
            device_id=to, device_id_type=MESH,
        )

    def up(aa, h):
        return send_x(aa, me, h, z_send.at[0, aa, h], dev(lax.rem(a + 1, outer), i, me))

    def down(aa, h):
        return send_x(aa, me, h, z_send.at[1, aa, h], dev(lax.rem(a + outer - 1, outer), i, me))

    def across(aa, k, h):
        to = dev(a, i, lax.rem(y + k, ys) * 2 + c)
        return send_x(aa, me, h, y_send.at[aa, k - 1, h], to)

    def sibling(aa, yy, h):
        return send_x(aa, yy * 2 + c, h, core_send.at[aa, yy, h], dev(a, i, partner))

    def arrived(aa, pp, h):
        send_x(aa, pp, h, z_send.at[0, aa, h], dev(a, i, partner)).wait_recv()

    def goes_up(aa):
        return (aa <= a) & (a + 1 < outer)

    def goes_down(aa):
        return (aa >= a) & (a > 0)

    def send_w(k, t):
        return pltpu.make_async_remote_copy(
            src_ref=w_buf.at[i, t], dst_ref=w_buf.at[i, t],
            send_sem=w_send.at[k - 1, t], recv_sem=w_recv.at[i, t],
            device_id=dev(a, lax.rem(i + k, inner), me), device_id_type=MESH,
        )

    def send_c(k):
        return pltpu.make_async_remote_copy(
            src_ref=c_buf.at[i], dst_ref=c_buf.at[i],
            send_sem=c_send.at[k - 1], recv_sem=c_recv.at[i],
            device_id=dev(a, lax.rem(i + k, inner), me), device_id_type=MESH,
        )

    def nth(j):
        low = jnp.minimum(a, outer - 1 - a)
        near = jnp.where(j % 2 == 1, a - (j + 1) // 2, a + j // 2)
        far = jnp.where(a < outer - 1 - a, j, outer - 1 - j)
        return jnp.where(j <= 2 * low, near, far)

    def spread(aa, first):
        for h in range(PIECES):
            if not first:
                arrived(aa, me, h)
            pl.when(goes_up(aa))(lambda h=h: up(aa, h).start())
            pl.when(goes_down(aa))(lambda h=h: down(aa, h).start())
            for k in range(1, ys):
                across(aa, k, h).start()
            sibling(aa, y, h).start()

    def pass_on(aa):
        for k in range(1, ys):
            yy = lax.rem(y + k, ys)
            for h in range(PIECES):
                arrived(aa, yy * 2 + c, h)
                sibling(aa, yy, h).start()

    def settle(aa, yy):
        for h in range(PIECES):
            arrived(aa, yy * 2 + (1 - c), h)

    n_steps, per_step, _ = hbias_ref.shape
    span = 2 * rows
    cols = STEP_COLS if span % STEP_COLS == 0 else span

    def compute(aa, yy, ii):
        def body(s, _):
            t0 = s * per_step
            w = w_buf[ii, pl.ds(t0, per_step)].reshape(per_step * hidden, depth)
            bias = c_buf[ii, 0, pl.ds(t0, per_step)].reshape(per_step * hidden, LANES)
            head = c_buf[ii, 1, pl.ds(t0, per_step)].reshape(per_step * hidden, LANES)
            bias = bias.astype(jnp.float32)
            head = head.astype(jnp.float32)
            for n in range(span // cols):
                at = pl.ds(pl.multiple_of(yy * span + n * cols, LANES), cols)
                pre = lax.dot_general(
                    w, x_buf[aa, at], (((1,), (1,)), ((), ())),
                    preferred_element_type=jnp.float32,
                )
                for l in range(cols // LANES):
                    tile = n * cols + l * LANES
                    v = jnp.maximum(pre[:, l * LANES : (l + 1) * LANES] + bias, 0.0) * head
                    for t in range(per_step):
                        total = jnp.sum(v[t * hidden : (t + 1) * hidden], axis=0, keepdims=True)
                        lane = pl.ds(tile % rows, LANES)
                        part[aa, yy * 2 + tile // rows, s, pl.ds(t, 1), lane] += total
            return 0

        lax.fori_loop(0, n_steps, body, 0)

    def send_part(aa, pp):
        return pltpu.make_async_remote_copy(
            src_ref=part.at[aa, pp], dst_ref=ret.at[a, me],
            send_sem=p_send.at[aa, pp], recv_sem=p_recv.at[a, me],
            device_id=dev(aa, i, pp), device_id_type=MESH,
        )

    def give_back(aa, yy):
        for cc in range(2):
            pp = yy * 2 + cc
            mine = (aa == a) & (pp == me)
            pl.when(jnp.logical_not(mine))(lambda pp=pp: send_part(aa, pp).start())

    spread(a, True)
    for k in range(1, inner):
        send_c(k).start()
        for t in range(towers):
            send_w(k, t).start()

    settle(a, y)
    compute(a, y, i)

    def round_(j, _):
        aa, before = nth(j), nth(j - 1)
        spread(aa, False)
        pass_on(before)
        for k in range(1, ys):
            yy = lax.rem(y + k, ys)
            settle(before, yy)
            compute(before, yy, i)
        settle(aa, y)
        compute(aa, y, i)
        return 0

    lax.fori_loop(1, outer, round_, 0)

    def w_arrived(k):
        ii = lax.rem(i + k, inner)
        pltpu.make_async_remote_copy(
            src_ref=c_buf.at[ii], dst_ref=c_buf.at[ii], send_sem=c_send.at[0],
            recv_sem=c_recv.at[ii], device_id=dev(a, ii, me), device_id_type=MESH,
        ).wait_recv()
        for t in range(towers):
            pltpu.make_async_remote_copy(
                src_ref=w_buf.at[ii, t], dst_ref=w_buf.at[ii, t], send_sem=w_send.at[0, t],
                recv_sem=w_recv.at[ii, t], device_id=dev(a, ii, me), device_id_type=MESH,
            ).wait_recv()

    for k in range(1, inner):
        w_arrived(k)

    def rest(aa, yy):
        def one(k, _):
            compute(aa, yy, lax.rem(i + k, inner))
            return 0

        lax.fori_loop(1, inner, one, 0)
        give_back(aa, yy)

    def early(q, _):
        j, k = q // ys, q % ys
        rest(nth(j), lax.rem(y + k, ys))
        return 0

    last = nth(outer - 1)
    lax.fori_loop(0, (outer - 1) * ys, early, 0)
    rest(last, y)
    pass_on(last)
    for k in range(1, ys):
        yy = lax.rem(y + k, ys)
        settle(last, yy)
        compute(last, yy, i)
        rest(last, yy)

    def landed(aa, pp):
        pltpu.make_async_remote_copy(
            src_ref=part.at[aa, pp], dst_ref=ret.at[aa, pp], send_sem=p_send.at[aa, pp],
            recv_sem=p_recv.at[aa, pp], device_id=dev(a, i, partner), device_id_type=MESH,
        ).wait_recv()

    ret[a, me] = part[a, me]
    for aa in range(outer):
        for pp in range(peers):
            mine = (a == aa) & (me == pp)
            pl.when(jnp.logical_not(mine))(lambda aa=aa, pp=pp: landed(aa, pp))
    for pp in range(peers):
        total = ret[0, pp]
        for aa in range(1, outer):
            total += ret[aa, pp]
        out_ref[pp] = total

    for aa in range(outer):
        for h in range(PIECES):
            pl.when(goes_up(aa))(lambda aa=aa, h=h: up(aa, h).wait_send())
            pl.when(goes_down(aa))(lambda aa=aa, h=h: down(aa, h).wait_send())
            for k in range(1, ys):
                across(aa, k, h).wait_send()
            for yy in range(ys):
                sibling(aa, yy, h).wait_send()
        for pp in range(peers):
            mine = (a == aa) & (me == pp)
            pl.when(jnp.logical_not(mine))(lambda aa=aa, pp=pp: send_part(aa, pp).wait_send())
    for k in range(1, inner):
        send_c(k).wait_send()
        for t in range(towers):
            send_w(k, t).wait_send()


def shards(features, task_mask, tower_in, tower_bias, tower_head, head_bias):
    peers, group = lax.axis_size("peer"), lax.axis_size("group")
    rows, depth = features.shape
    towers, hidden, _ = tower_in.shape
    inner = split_of_group(group, peers, tower_in.size, features.size)
    outer = group // inner
    ys = peers // 2
    columns = jnp.stack([tower_bias, tower_head])[..., None]
    columns = jnp.broadcast_to(columns, (2, towers, hidden, LANES))
    per_step = max(n for n in range(1, towers + 1) if towers % n == 0 and n * hidden <= STEP_ROWS)
    steps = (towers // per_step, per_step)
    start = jnp.broadcast_to(head_bias.reshape(steps)[..., None], (*steps, rows))
    dma = pltpu.SemaphoreType.DMA
    logits = pl.pallas_call(
        functools.partial(kernel, outer, inner, peers),
        out_shape=jax.ShapeDtypeStruct((peers, *steps, rows), jnp.float32),
        in_specs=[pl.BlockSpec(memory_space=pl.ANY)] * 3
        + [pl.BlockSpec(memory_space=pltpu.VMEM)],
        out_specs=pl.BlockSpec(memory_space=pltpu.VMEM),
        scratch_shapes=[
            pltpu.VMEM((outer, peers * rows, depth), features.dtype),
            pltpu.VMEM((inner, towers, hidden, depth), tower_in.dtype),
            pltpu.VMEM((inner, 2, towers, hidden, LANES), tower_bias.dtype),
            pltpu.VMEM((outer, peers, *steps, rows), jnp.float32),
            pltpu.VMEM((outer, peers, *steps, rows), jnp.float32),
            dma((3,)),
            dma((outer, peers, PIECES)),
            dma((2, outer, PIECES)),
            dma((outer, max(1, ys - 1), PIECES)),
            dma((outer, ys, PIECES)),
            dma((max(1, inner - 1), towers)),
            dma((inner, towers)),
            dma((max(1, inner - 1),)),
            dma((inner,)),
            dma((outer, peers)),
            dma((outer, peers)),
        ],
        compiler_params=pltpu.CompilerParams(
            collective_id=0, has_side_effects=True, vmem_limit_bytes=60 * 1024 * 1024
        ),
    )(features, tower_in, columns, start)
    tasks = jnp.arange(peers * towers, dtype=jnp.int32)
    bits = (task_mask[:, None] >> tasks[None, :]) & 1
    return jnp.where(bits == 1, logits.reshape(peers * towers, rows).T, 0.0)


def solution(mesh):
    placed = (
        P(("group", "peer"), None),
        P(("group", "peer")),
        P("peer", "group", None),
        P("peer", "group"),
        P("peer", "group"),
        P("peer"),
    )
    return jax.shard_map(
        shards, mesh=mesh, in_specs=placed, out_specs=P(("group", "peer"), None), check_vma=False
    )
```

```python
import functools

import jax
import jax.numpy as jnp
from jax import lax
from jax.experimental import pallas as pl
from jax.experimental.pallas import tpu as pltpu
from jax.sharding import PartitionSpec as P

MESH = pl.DeviceIdType.MESH
LANES = 128
PIECE_ROWS = 64
FIRST = 0
STEP_COLS = 256


def split_of_group(group, peers, weight_bytes, sample_bytes):
    sizes = [f for f in range(1, group + 1) if group % f == 0]

    def cost(f):
        return (f - 1) * weight_bytes + (group // f * peers - 1) * sample_bytes / 2

    return min(sizes, key=cost)


def kernel(
    outer, inner, peers,
    feat_ref, weight_ref, bias_ref, head_ref, hbias_ref, out_ref,
    x_buf, w_buf, b_buf, c_buf, part, ret,
    load_sem, x_recv, z_send, f_send, y_send, core_send, w_send, w_recv, b_send, b_recv,
    p_send, p_recv,
):
    rows, depth = feat_ref.shape
    towers, hidden, _ = weight_ref.shape
    piece = PIECE_ROWS
    pieces = rows // piece
    ys = peers // 2
    group_at, me = lax.axis_index("group"), lax.axis_index("peer")
    a, i = group_at // inner, group_at % inner
    y, c = me // 2, me % 2
    partner = y * 2 + (1 - c)

    def dev(a_to, i_to, p_to):
        return (a_to * inner + i_to, p_to)

    load_x = pltpu.make_async_copy(
        feat_ref, x_buf.at[a, pl.ds(pl.multiple_of(me * rows, rows), rows)], load_sem.at[0]
    )
    load_w = pltpu.make_async_copy(weight_ref, w_buf.at[i], load_sem.at[1])
    load_b = pltpu.make_async_copy(bias_ref, b_buf.at[i, 0], load_sem.at[2])
    load_h = pltpu.make_async_copy(head_ref, b_buf.at[i, 1], load_sem.at[3])
    load_x.start()
    load_w.start()
    load_b.start()
    load_h.start()

    barrier = pltpu.get_barrier_semaphore()
    others = outer * peers - 1

    def greet(k, _):
        at = lax.rem(a * peers + me + k, outer * peers)
        pl.semaphore_signal(
            barrier, inc=1, device_id=dev(at // peers, i, at % peers), device_id_type=MESH
        )
        return 0

    lax.fori_loop(1, others + 1, greet, 0)
    for k in range(1, inner):
        pl.semaphore_signal(
            barrier, inc=1, device_id=dev(a, lax.rem(i + k, inner), me), device_id_type=MESH
        )

    for t in range(towers):
        start = jnp.where(a == 0, hbias_ref[t], 0.0)
        for aa in range(outer):
            for pp in range(peers):
                part[aa, pp, pl.ds(t, 1)] = jnp.full((1, rows), start, jnp.float32)

    load_x.wait()
    load_w.wait()
    load_b.wait()
    load_h.wait()
    pl.semaphore_wait(barrier, others + inner - 1)

    def x_piece(aa, pp, h):
        return x_buf.at[aa, pl.ds(pl.multiple_of(pp * rows + h * piece, piece), piece)]

    def send_x(aa, pp, h, sem, to):
        ref = x_piece(aa, pp, h)
        return pltpu.make_async_remote_copy(
            src_ref=ref, dst_ref=ref, send_sem=sem, recv_sem=x_recv.at[aa, pp, h],
            device_id=to, device_id_type=MESH,
        )

    def up(aa, h):
        return send_x(aa, me, h, z_send.at[0, aa, h], dev(lax.rem(a + 1, outer), i, me))

    def down(aa, h):
        return send_x(aa, me, h, z_send.at[1, aa, h], dev(lax.rem(a + outer - 1, outer), i, me))

    def across(aa, k, h):
        to = dev(a, i, lax.rem(y + k, ys) * 2 + c)
        return send_x(aa, me, h, y_send.at[aa, k - 1, h], to)

    def sibling(aa, yy, h):
        return send_x(aa, yy * 2 + c, h, core_send.at[aa, yy, h], dev(a, i, partner))

    def arrived(aa, pp, h):
        send_x(aa, pp, h, z_send.at[0, aa, h], dev(a, i, partner)).wait_recv()

    def goes_up(aa):
        return (aa <= a) & (a + 1 < outer)

    def goes_down(aa):
        return (aa >= a) & (a > 0)

    def send_w(k, t):
        return pltpu.make_async_remote_copy(
            src_ref=w_buf.at[i, t], dst_ref=w_buf.at[i, t],
            send_sem=w_send.at[k - 1, t], recv_sem=w_recv.at[i, t],
            device_id=dev(a, lax.rem(i + k, inner), me), device_id_type=MESH,
        )

    def send_b(k):
        return pltpu.make_async_remote_copy(
            src_ref=b_buf.at[i], dst_ref=b_buf.at[i],
            send_sem=b_send.at[k - 1], recv_sem=b_recv.at[i],
            device_id=dev(a, lax.rem(i + k, inner), me), device_id_type=MESH,
        )

    def columns(ii):
        diagonal = lax.broadcasted_iota(jnp.int32, (hidden, hidden), 0) == (
            lax.broadcasted_iota(jnp.int32, (hidden, hidden), 1)
        )
        for w in range(2):
            both = b_buf[ii, w].astype(jnp.float32)
            for t in range(towers):
                picked = jnp.where(diagonal, both[t : t + 1], 0.0)
                column = jnp.sum(picked, axis=1, keepdims=True)
                c_buf[ii, w, t] = jnp.broadcast_to(column, (hidden, LANES))

    def nth(j):
        low = jnp.minimum(a, outer - 1 - a)
        near = jnp.where(j % 2 == 1, a - (j + 1) // 2, a + j // 2)
        far = jnp.where(a < outer - 1 - a, j, outer - 1 - j)
        return jnp.where(j <= 2 * low, near, far)

    def cross_first(aa, k, d):
        pp = lax.rem(y + k, ys) * 2 + c
        to = dev(lax.rem(a + outer + 1 - 2 * d, outer), i, me)
        return send_x(aa, pp, FIRST, f_send.at[d, aa, k - 1], to)

    def spread(aa, h, own):
        if not own:
            arrived(aa, me, h)
        pl.when(goes_up(aa))(lambda: up(aa, h).start())
        pl.when(goes_down(aa))(lambda: down(aa, h).start())
        if own or h != FIRST:
            for k in range(1, ys):
                across(aa, k, h).start()
        sibling(aa, y, h).start()

    def pass_on(aa, h):
        for k in range(1, ys):
            yy = lax.rem(y + k, ys)
            arrived(aa, yy * 2 + c, h)
            if h == FIRST:
                pl.when(goes_up(aa))(lambda k=k: cross_first(aa, k, 0).start())
                pl.when(goes_down(aa))(lambda k=k: cross_first(aa, k, 1).start())
            sibling(aa, yy, h).start()

    def settle(aa, yy):
        for h in range(pieces):
            arrived(aa, yy * 2 + (1 - c), h)

    span = 2 * rows
    cols = STEP_COLS if span % STEP_COLS == 0 else span

    def compute(aa, yy, ii, t0, t1):
        count = (t1 - t0) * hidden
        w = w_buf[ii, t0:t1].reshape(count, depth)
        bias = c_buf[ii, 0, t0:t1].reshape(count, LANES)
        head = c_buf[ii, 1, t0:t1].reshape(count, LANES)
        for n in range(span // cols):
            at = pl.ds(pl.multiple_of(yy * span + n * cols, LANES), cols)
            pre = lax.dot_general(
                w, x_buf[aa, at], (((1,), (1,)), ((), ())),
                preferred_element_type=jnp.float32,
            )
            for l in range(cols // LANES):
                tile = n * cols + l * LANES
                lane = pl.ds(tile % rows, LANES)
                v = jnp.maximum(pre[:, l * LANES : (l + 1) * LANES] + bias, 0.0) * head
                for t in range(t1 - t0):
                    total = jnp.sum(v[t * hidden : (t + 1) * hidden], axis=0, keepdims=True)
                    part[aa, yy * 2 + tile // rows, pl.ds(t0 + t, 1), lane] += total

    def send_part(aa, pp):
        return pltpu.make_async_remote_copy(
            src_ref=part.at[aa, pp], dst_ref=ret.at[a, me],
            send_sem=p_send.at[aa, pp], recv_sem=p_recv.at[a, me],
            device_id=dev(aa, i, pp), device_id_type=MESH,
        )

    def give_back(aa, yy):
        for cc in range(2):
            pp = yy * 2 + cc
            mine = (aa == a) & (pp == me)
            pl.when(jnp.logical_not(mine))(lambda pp=pp: send_part(aa, pp).start())

    def pair(u):
        return nth(u // ys), lax.rem(y + u % ys, ys)

    far = max(inner - 1, 1)
    half = towers // 2

    def own_jobs(u1):
        for u in range(done[0], u1):
            settle(*pair(u))

        def job(u, _):
            compute(*pair(u), i, 0, towers)
            return 0

        if u1 > done[0]:
            lax.fori_loop(done[0], u1, job, 0)
        done[0] = max(done[0], u1)

    def far_jobs(v0, v1, t0, t1):
        def job(q, _):
            compute(*pair(q // far), lax.rem(i + 1 + q % far, inner), t0, t1)
            return 0

        if v1 > v0 and inner > 1:
            lax.fori_loop(v0 * far, v1 * far, job, 0)
        if t1 == towers:
            for v in range(v0, v1):
                give_back(*pair(v))

    def low_jobs(v1):
        v1 = min(v1, done[0])
        far_jobs(done[1], v1, 0, half)
        done[1] = max(done[1], v1)

    def high_jobs(v1):
        v1 = min(v1, done[1])
        far_jobs(done[2], v1, half, towers)
        done[2] = max(done[2], v1)

    for h in range(pieces):
        spread(a, h, True)
    for k in range(1, inner):
        send_b(k).start()
        for t in range(towers):
            send_w(k, t).start()
    columns(i)

    def weights_arrived(part_of):
        if part_of in got:
            return
        got.add(part_of)
        for k in range(1, inner):
            ii = lax.rem(i + k, inner)
            if part_of == 0:
                pltpu.make_async_remote_copy(
                    src_ref=b_buf.at[ii], dst_ref=b_buf.at[ii], send_sem=b_send.at[0],
                    recv_sem=b_recv.at[ii], device_id=dev(a, ii, me), device_id_type=MESH,
                ).wait_recv()
                columns(ii)
            for t in range(half) if part_of == 0 else range(half, towers):
                pltpu.make_async_remote_copy(
                    src_ref=w_buf.at[ii, t], dst_ref=w_buf.at[ii, t], send_sem=w_send.at[0, t],
                    recv_sem=w_recv.at[ii, t], device_id=dev(a, ii, me), device_id_type=MESH,
                ).wait_recv()

    pairs = outer * ys
    done, got = [0, 0, 0], set()
    own_jobs(1)
    for j in range(1, outer):
        aa, before = nth(j), nth(j - 1)
        passed = 0
        window = pieces if j == 1 else max(1, pieces - 2)
        for h in range(pieces):
            spread(aa, h, False)
            upto = min(pieces, -(-pieces * (h + 1) // window))
            for g in range(passed, upto):
                pass_on(before, g)
            passed = upto
            if upto == pieces:
                own_jobs(j * ys)
            late = h >= window - 1
            if (j == outer - 2 and late) or j == outer - 1:
                weights_arrived(0)
                low_jobs(done[1] + 1)
            if j == outer - 1 and late:
                weights_arrived(1)
                high_jobs(done[2] + 2)
        if j < outer - 1:
            own_jobs(j * ys + 1)
    weights_arrived(0)
    weights_arrived(1)
    last = nth(outer - 1)
    for h in range(pieces - 2):
        pass_on(last, h)
    own_jobs((outer - 1) * ys + 1)
    for h in range(max(0, pieces - 2), pieces):
        pass_on(last, h)
    low_jobs(done[0])
    high_jobs(done[1])
    for u in range(done[0], pairs):
        own_jobs(u + 1)
        far_jobs(u, u + 1, 0, towers)

    def landed(aa, pp):
        pltpu.make_async_remote_copy(
            src_ref=part.at[aa, pp], dst_ref=ret.at[aa, pp], send_sem=p_send.at[aa, pp],
            recv_sem=p_recv.at[aa, pp], device_id=dev(a, i, partner), device_id_type=MESH,
        ).wait_recv()

    ret[a, me] = part[a, me]
    for aa in range(outer):
        for pp in range(peers):
            mine = (a == aa) & (me == pp)
            pl.when(jnp.logical_not(mine))(lambda aa=aa, pp=pp: landed(aa, pp))
    for pp in range(peers):
        total = ret[0, pp]
        for aa in range(1, outer):
            total += ret[aa, pp]
        out_ref[pp] = total

    for aa in range(outer):
        for h in range(pieces):
            pl.when(goes_up(aa))(lambda aa=aa, h=h: up(aa, h).wait_send())
            pl.when(goes_down(aa))(lambda aa=aa, h=h: down(aa, h).wait_send())
            for k in range(1, ys):
                sent = (a == aa) | (h != FIRST)
                pl.when(sent)(lambda aa=aa, k=k, h=h: across(aa, k, h).wait_send())
            for yy in range(ys):
                sibling(aa, yy, h).wait_send()
        for k in range(1, ys):
            pl.when(goes_up(aa))(lambda aa=aa, k=k: cross_first(aa, k, 0).wait_send())
            pl.when(goes_down(aa))(lambda aa=aa, k=k: cross_first(aa, k, 1).wait_send())
        for pp in range(peers):
            mine = (a == aa) & (me == pp)
            pl.when(jnp.logical_not(mine))(lambda aa=aa, pp=pp: send_part(aa, pp).wait_send())
    for k in range(1, inner):
        send_b(k).wait_send()
        for t in range(towers):
            send_w(k, t).wait_send()


def shards(features, task_mask, tower_in, tower_bias, tower_head, head_bias):
    peers, group = lax.axis_size("peer"), lax.axis_size("group")
    rows, depth = features.shape
    towers, hidden, _ = tower_in.shape
    inner = split_of_group(group, peers, tower_in.size, features.size)
    outer = group // inner
    ys = peers // 2
    pieces = rows // PIECE_ROWS
    dma = pltpu.SemaphoreType.DMA
    logits = pl.pallas_call(
        functools.partial(kernel, outer, inner, peers),
        out_shape=jax.ShapeDtypeStruct((peers, towers, rows), jnp.float32),
        in_specs=[pl.BlockSpec(memory_space=pl.ANY)] * 4
        + [pl.BlockSpec(memory_space=pltpu.SMEM)],
        out_specs=pl.BlockSpec(memory_space=pltpu.VMEM),
        scratch_shapes=[
            pltpu.VMEM((outer, peers * rows, depth), features.dtype),
            pltpu.VMEM((inner, towers, hidden, depth), tower_in.dtype),
            pltpu.VMEM((inner, 2, towers, hidden), tower_bias.dtype),
            pltpu.VMEM((inner, 2, towers, hidden, LANES), jnp.float32),
            pltpu.VMEM((outer, peers, towers, rows), jnp.float32),
            pltpu.VMEM((outer, peers, towers, rows), jnp.float32),
            dma((4,)),
            dma((outer, peers, pieces)),
            dma((2, outer, pieces)),
            dma((2, outer, max(1, ys - 1))),
            dma((outer, max(1, ys - 1), pieces)),
            dma((outer, ys, pieces)),
            dma((max(1, inner - 1), towers)),
            dma((inner, towers)),
            dma((max(1, inner - 1),)),
            dma((inner,)),
            dma((outer, peers)),
            dma((outer, peers)),
        ],
        compiler_params=pltpu.CompilerParams(
            collective_id=0, has_side_effects=True, vmem_limit_bytes=60 * 1024 * 1024
        ),
    )(features, tower_in, tower_bias, tower_head, head_bias)
    tasks = jnp.arange(peers * towers, dtype=jnp.int32)
    bits = (task_mask[:, None] >> tasks[None, :]) & 1
    return jnp.where(bits == 1, logits.reshape(peers * towers, rows).T, 0.0)


def solution(mesh):
    placed = (
        P(("group", "peer"), None),
        P(("group", "peer")),
        P("peer", "group", None),
        P("peer", "group"),
        P("peer", "group"),
        P("peer"),
    )
    return jax.shard_map(
        shards, mesh=mesh, in_specs=placed, out_specs=P(("group", "peer"), None), check_vma=False
    )
```
